128 devices in a mesh: dp: 1, cp: 128 (over z, y, x, core).
Axes of the slice: x: 4, y: 4, z: 4, core: 2. Of those that a mesh axis runs over, the one named last changes fastest.
Arguments:
- q_rope: bfloat16 [1, 65536, 12, 128], P('dp', 'cp')
- k_rope: bfloat16 [1, 65536, 2, 128], P('dp', 'cp')
- values: bfloat16 [1, 65536, 2, 128], P('dp', 'cp')
- d_out: bfloat16 [1, 65536, 12, 128], P('dp', 'cp')
Outputs:
- output 1: bfloat16 [1, 65536, 12, 128], P('dp', 'cp')
- output 2: bfloat16 [1, 65536, 12, 128], P('dp', 'cp')
- output 3: bfloat16 [1, 65536, 2, 128], P('dp', 'cp')
- output 4: bfloat16 [1, 65536, 2, 128], P('dp', 'cp')
All inputs are finite; a program needn't handle non-finite values.
Results may differ from the reference program's by a relative error of at most 0.00898008.
Values are sent between devices in bfloat16 or wider.
A program may use at most 1 GiB of HBM per device.

```python
import jax
import jax.numpy as jnp
from jax import lax

BATCH = 1
SEQ = 65536
HEADS = 12
KV_HEADS = 2
HEAD = 128
BLOCK = 64
LOCAL = 16
STRIDE = 8

GROUP = HEADS // KV_HEADS
HALO = (LOCAL - 1) * BLOCK
WINDOW = LOCAL * BLOCK
SCALE = 1.0 / HEAD


def setup_inputs(seed: int = 0, part: int = 0) -> dict:
    rng_key = jax.random.fold_in(jax.random.key(seed), part)
    key_q, key_k, key_v, key_d = jax.random.split(rng_key, 4)
    qk_std = 1.6 * HEAD ** 0.25
    q_shape = (BATCH, SEQ, HEADS, HEAD)
    kv_shape = (BATCH, SEQ, KV_HEADS, HEAD)
    q_rope = (qk_std * jax.random.normal(key_q, q_shape, jnp.float32)).astype(jnp.bfloat16)
    k_rope = (qk_std * jax.random.normal(key_k, kv_shape, jnp.float32)).astype(jnp.bfloat16)
    values = jax.random.normal(key_v, kv_shape, jnp.float32).astype(jnp.bfloat16)
    d_out = jax.random.normal(key_d, q_shape, jnp.float32).astype(jnp.bfloat16)
    return {'q_rope': q_rope, 'k_rope': k_rope, 'values': values, 'd_out': d_out}


def residue_table():
    head_ids = jnp.arange(KV_HEADS)[:, None] * GROUP + jnp.arange(GROUP)[None, :]
    return (-1 - head_ids) % STRIDE


def select_matrix():
    return (jnp.arange(STRIDE)[None, None, :] == residue_table()[:, :, None]).astype(jnp.float32)


def compact(keys_in):
    grouped = keys_in.astype(jnp.float32).reshape(BATCH, SEQ // (BLOCK * STRIDE), STRIDE, BLOCK, KV_HEADS, HEAD)
    picked = jnp.einsum('bmsigd,gus->bmigud', grouped, select_matrix())
    return picked.reshape(BATCH, SEQ // STRIDE, KV_HEADS, GROUP, HEAD)


def expand(grads):
    grouped = grads.reshape(BATCH, SEQ // (BLOCK * STRIDE), BLOCK, KV_HEADS, GROUP, HEAD)
    spread = jnp.einsum('bmigud,gus->bmsigd', grouped, select_matrix())
    return spread.reshape(BATCH, SEQ, KV_HEADS, HEAD)


def block_pass(q_rope, d_out, k_ext, v_ext, k_str, v_str):
    str_block = (jnp.arange(SEQ // STRIDE) // BLOCK)[None, None, :] * STRIDE + residue_table()[:, :, None]
    row_ids = jnp.arange(BLOCK)[:, None]
    col_ids = jnp.arange(WINDOW)[None, :]
    blk_shape = (BATCH, BLOCK, KV_HEADS, GROUP, HEAD)

    def body(carry, blk_idx):
        dk_ext, dv_ext, dk_str, dv_str = carry
        win_start = blk_idx * BLOCK
        q_blk = lax.dynamic_slice_in_dim(q_rope, win_start, BLOCK, axis=1).astype(jnp.float32).reshape(blk_shape)
        do_blk = lax.dynamic_slice_in_dim(d_out, win_start, BLOCK, axis=1).astype(jnp.float32).reshape(blk_shape)
        k_win = lax.dynamic_slice_in_dim(k_ext, win_start, WINDOW, axis=1)
        v_win = lax.dynamic_slice_in_dim(v_ext, win_start, WINDOW, axis=1)
        loc_mask = (col_ids <= row_ids + HALO) & (col_ids >= HALO - blk_idx * BLOCK)
        str_mask = (str_block <= blk_idx - LOCAL)[:, :, None, :]
        s_loc = jnp.where(loc_mask, jnp.einsum('bigud,bjgd->bguij', q_blk, k_win) * SCALE, -jnp.inf)
        s_str = jnp.where(str_mask, jnp.einsum('bigud,bjgud->bguij', q_blk, k_str) * SCALE, -jnp.inf)
        row_max = jnp.maximum(jnp.max(s_loc, axis=-1), jnp.max(s_str, axis=-1))[..., None]
        e_loc = jnp.exp(s_loc - row_max)
        e_str = jnp.exp(s_str - row_max)
        row_sum = jnp.sum(e_loc, axis=-1, keepdims=True) + jnp.sum(e_str, axis=-1, keepdims=True)
        p_loc = e_loc / row_sum
        p_str = e_str / row_sum
        pb_loc = p_loc.astype(jnp.bfloat16).astype(jnp.float32)
        pb_str = p_str.astype(jnp.bfloat16).astype(jnp.float32)
        o_blk = jnp.einsum('bguij,bjgd->bigud', pb_loc, v_win) + jnp.einsum('bguij,bjgud->bigud', pb_str, v_str)
        row_delta = jnp.einsum('bigud,bigud->bgui', do_blk, o_blk)[..., None]
        dp_loc = jnp.einsum('bigud,bjgd->bguij', do_blk, v_win)
        dp_str = jnp.einsum('bigud,bjgud->bguij', do_blk, v_str)
        ds_loc = (p_loc * (dp_loc - row_delta)).astype(jnp.bfloat16).astype(jnp.float32)
        ds_str = (p_str * (dp_str - row_delta)).astype(jnp.bfloat16).astype(jnp.float32)
        dq_blk = (jnp.einsum('bguij,bjgd->bigud', ds_loc, k_win) + jnp.einsum('bguij,bjgud->bigud', ds_str, k_str)) * SCALE
        dk_win = jnp.einsum('bguij,bigud->bjgd', ds_loc, q_blk) * SCALE
        dv_win = jnp.einsum('bguij,bigud->bjgd', pb_loc, do_blk)
        dk_ext = lax.dynamic_update_slice_in_dim(dk_ext, lax.dynamic_slice_in_dim(dk_ext, win_start, WINDOW, axis=1) + dk_win, win_start, axis=1)
        dv_ext = lax.dynamic_update_slice_in_dim(dv_ext, lax.dynamic_slice_in_dim(dv_ext, win_start, WINDOW, axis=1) + dv_win, win_start, axis=1)
        dk_str = dk_str + jnp.einsum('bguij,bigud->bjgud', ds_str, q_blk) * SCALE
        dv_str = dv_str + jnp.einsum('bguij,bigud->bjgud', pb_str, do_blk)
        return (dk_ext, dv_ext, dk_str, dv_str), (o_blk.astype(jnp.bfloat16), dq_blk.astype(jnp.bfloat16))

    init = (jnp.zeros(k_ext.shape, jnp.float32), jnp.zeros(v_ext.shape, jnp.float32), jnp.zeros(k_str.shape, jnp.float32), jnp.zeros(v_str.shape, jnp.float32))
    carry, stacked = lax.scan(body, init, jnp.arange(SEQ // BLOCK))
    attn_out = jnp.moveaxis(stacked[0], 0, 1).reshape(BATCH, SEQ, HEADS, HEAD)
    d_q = jnp.moveaxis(stacked[1], 0, 1).reshape(BATCH, SEQ, HEADS, HEAD)
    return (attn_out, d_q) + carry


def reference(q_rope, k_rope, values, d_out):
    pad_widths = ((0, 0), (HALO, 0), (0, 0), (0, 0))
    k_ext = jnp.pad(k_rope, pad_widths).astype(jnp.float32)
    v_ext = jnp.pad(values, pad_widths).astype(jnp.float32)
    attn_out, d_q, dk_ext, dv_ext, dk_str, dv_str = block_pass(q_rope, d_out, k_ext, v_ext, compact(k_rope), compact(values))
    d_k = dk_ext[:, HALO:] + expand(dk_str)
    d_v = dv_ext[:, HALO:] + expand(dv_str)
    return (attn_out, d_q, d_k.astype(jnp.bfloat16), d_v.astype(jnp.bfloat16))
```

```python
import functools
import math

import jax
import jax.numpy as jnp
from jax import lax
from jax.experimental import pallas as pl
from jax.experimental.pallas import tpu as pltpu
from jax.sharding import PartitionSpec as P


BLOCK = 64
LOCAL = 16
STRIDE = 8
NX = 4
TRIPLE = 3
HALF = 256
RUN = 512
HALO = 1024
CHUNK = 512
F32 = jnp.float32
BF16 = jnp.bfloat16


def dev(z, y, x, c):
    return ((z * 4 + y) * NX + x) * 2 + c


def zof(zp, zm):
    return zp if zm == 0 else 3 - zp


GROUP_Q = [[dev(zof(zp, zm), y, x, c) for zm in range(2) for x in range(NX)] for zp in range(2) for y in range(4) for c in range(2)]
GROUP_X = [[dev(z, y, x, c) for x in range(NX)] for z in range(4) for y in range(4) for c in range(2)]
GROUP_ZYC = [[dev(z, y, x, c) for z in range(4) for y in range(4) for c in range(2)] for x in range(NX)]
GROUP_WG = [[dev(zof(zp, zm), y, 2 * xh + xl, c) for zm in range(2) for xl in range(2) for c in range(2)] for zp in range(2) for y in range(4) for xh in range(2)]
GROUP_W = [[dev(zof(zp, zm), y, x, c) for zm in range(2) for x in range(NX) for c in range(2)] for zp in range(2) for y in range(4)]


def residue(head):
    return (-1 - head) % STRIDE


def nt(a, b):
    return lax.dot_general(a, b, (((1,), (1,)), ((), ())), preferred_element_type=F32)


def tn(a, b):
    return lax.dot_general(a, b, (((0,), (0,)), ((), ())), preferred_element_type=F32)


def nn(a, b):
    return lax.dot_general(a, b, (((1,), (0,)), ((), ())), preferred_element_type=F32)


def attn_kernel(info, q_ref, do_ref, ks_ref, vs_ref, kw_ref, o_ref, dq_ref, dkv_ref, dkw_ref,
                e_s, dp_s, m_s, e_l, dp_l, dk_s, dv_s):
    tile = pl.program_id(0)
    member = tile // NX
    xsrc = tile % NX
    scale = 1.0 / 128
    cexp = scale * math.log2(math.e)
    group = info[member]
    core = info[2]
    half = info[3]
    res = info[4]
    t0 = RUN * (2 * xsrc + core) + HALF * half
    blk0 = group * 64 + t0 // BLOCK
    first_valid = HALO - (group * 4096 + t0)
    q = q_ref[0, 0]
    do = do_ref[0, 0]
    n_chunk = group + 1
    nl = (HALO + HALF) // HALF

    @pl.when(tile == 0)
    def _():
        dk_s[...] = jnp.zeros_like(dk_s)
        dv_s[...] = jnp.zeros_like(dv_s)

    @pl.when(xsrc == 0)
    def _():
        dkw_ref[...] = jnp.zeros_like(dkw_ref)

    qcol = lax.broadcasted_iota(jnp.int32, (HALF, HALF), 1)
    krow = lax.broadcasted_iota(jnp.int32, (HALF, HALF), 0)

    def win(i):
        return pl.ds(pl.multiple_of(t0 + i * HALF, HALF), HALF)

    m = jnp.full((1, HALF), -jnp.inf, F32)
    l = jnp.zeros((1, HALF), F32)
    for i in reversed(range(nl)):
        s = nt(kw_ref[0, 0, win(i)], q)
        ok = krow + i * HALF >= first_valid
        if i == 0:
            ok &= krow // BLOCK >= qcol // BLOCK + 1
        if i == nl - 1:
            ok &= krow <= qcol
        s = jnp.where(ok, s, -jnp.inf)
        m_new = jnp.maximum(m, jnp.max(s, axis=0, keepdims=True))
        e = jnp.exp2((s - m_new) * cexp)
        e_l[i] = e
        l = l * jnp.exp2((m - m_new) * cexp) + jnp.sum(e, axis=0, keepdims=True)
        m_s[16 + i] = jnp.broadcast_to(m_new, (8, HALF))
        m = m_new

    limit = blk0 - LOCAL - res

    def score(i, carry, masked):
        m, l = carry
        s = nt(ks_ref[pl.ds(2 * i, 2)].reshape(CHUNK, 128), q)
        if masked:
            kr = lax.broadcasted_iota(jnp.int32, (CHUNK, HALF), 0)
            qc = lax.broadcasted_iota(jnp.int32, (CHUNK, HALF), 1)
            run = 2 * ((kr // BLOCK) % NX) + kr // (BLOCK * NX)
            s = jnp.where(64 * i + 8 * run <= limit + qc // BLOCK, s, -jnp.inf)
        m_new = jnp.maximum(m, jnp.max(s, axis=0, keepdims=True))
        e = jnp.exp2((s - m_new) * cexp)
        e_s[i] = e
        l = l * jnp.exp2((m - m_new) * cexp) + jnp.sum(e, axis=0, keepdims=True)
        m_s[i] = jnp.broadcast_to(m_new, (8, HALF))
        return m_new, l

    carry = lax.fori_loop(0, jnp.maximum(group - 1, 0), functools.partial(score, masked=False), (m, l))
    m, l = lax.fori_loop(jnp.maximum(group - 1, 0), n_chunk, functools.partial(score, masked=True), carry)
    inv = 1.0 / l

    def factor(slot):
        return jnp.exp2((m_s[slot][0:1] - m) * cexp) * inv

    ot = jnp.zeros((128, HALF), F32)
    for i in range(nl):
        pb = (e_l[i] * factor(16 + i)).astype(BF16)
        v = kw_ref[0, 1, win(i)]
        ot += tn(v, pb)
        dkw_ref[0, 1, win(i)] += nn(pb, do)
        dp_l[i] = nt(v, do)

    def value(i, ot):
        pb = (e_s[i] * factor(i)).astype(BF16)
        v = vs_ref[pl.ds(2 * i, 2)].reshape(CHUNK, 128)
        rows = pl.ds(pl.multiple_of(i * CHUNK, CHUNK), CHUNK)
        dv_s[rows] += nn(pb, do)
        dp_s[i] = nt(v, do)
        return ot + tn(v, pb)

    ot = lax.fori_loop(0, n_chunk, value, ot)
    delta = jnp.sum(ot * do.astype(F32).T, axis=0, keepdims=True)
    o_ref[0] = ot.T.astype(BF16)

    dqt = jnp.zeros((128, HALF), F32)
    for i in range(nl):
        p = e_l[i] * factor(16 + i)
        ds = (p * (dp_l[i] - delta)).astype(BF16)
        dqt += tn(kw_ref[0, 0, win(i)], ds)
        dkw_ref[0, 0, win(i)] += nn(ds, q) * scale

    def grad(i, dqt):
        p = e_s[i] * factor(i)
        ds = (p * (dp_s[i] - delta)).astype(BF16)
        rows = pl.ds(pl.multiple_of(i * CHUNK, CHUNK), CHUNK)
        dk_s[rows] += nn(ds, q)
        return dqt + tn(ks_ref[pl.ds(2 * i, 2)].reshape(CHUNK, 128), ds)

    dqt = lax.fori_loop(0, n_chunk, grad, dqt)
    dq_ref[0] = (dqt * scale).T.astype(BF16)

    @pl.when(tile == pl.num_programs(0) - 1)
    def _():
        dkv_ref[:, 0] = (dk_s[...] * scale).astype(BF16).reshape(32, NX, BLOCK, 128)
        dkv_ref[:, 1] = dv_s[...].astype(BF16).reshape(32, NX, BLOCK, 128)


def head_attention(info, q_r, do_r, k_str, v_str, kv_win, u):
    whole = pl.BlockSpec((32, NX, BLOCK, 128), lambda t, s: (0, 0, 0, 0), pipeline_mode=pl.Buffered(1))
    qspec = pl.BlockSpec((1, 1, HALF, 128), lambda t, s: (t, u, 0, 0))
    ospec = pl.BlockSpec((1, HALF, 128), lambda t, s: (t, 0, 0))
    wspec = pl.BlockSpec((1, 2, HALO + 4096, 128), lambda t, s: (t // NX, 0, 0, 0))
    nslot = (HALO + HALF) // HALF
    pairs = 2048 * 5400
    return pl.pallas_call(
        attn_kernel,
        grid_spec=pltpu.PrefetchScalarGridSpec(
            num_scalar_prefetch=1,
            grid=(8,),
            in_specs=[qspec, qspec, whole, whole, wspec],
            out_specs=[ospec, ospec,
                       pl.BlockSpec((32, 2, NX, BLOCK, 128), lambda t, s: (0, 0, 0, 0, 0)),
                       wspec],
            scratch_shapes=[
                pltpu.VMEM((16, CHUNK, HALF), F32),
                pltpu.VMEM((16, CHUNK, HALF), F32),
                pltpu.VMEM((16 + nslot, 8, HALF), F32),
                pltpu.VMEM((nslot, HALF, HALF), F32),
                pltpu.VMEM((nslot, HALF, HALF), F32),
                pltpu.VMEM((8192, 128), F32),
                pltpu.VMEM((8192, 128), F32),
            ],
        ),
        out_shape=[jax.ShapeDtypeStruct((8, HALF, 128), BF16),
                   jax.ShapeDtypeStruct((8, HALF, 128), BF16),
                   jax.ShapeDtypeStruct((32, 2, NX, BLOCK, 128), BF16),
                   jax.ShapeDtypeStruct(kv_win.shape, F32)],
        compiler_params=pltpu.CompilerParams(vmem_limit_bytes=62 * 1024 * 1024),
        cost_estimate=pl.CostEstimate(flops=pairs * 6 * 256, bytes_accessed=40 * 1024 * 1024, transcendentals=pairs),
        name='head_attention',
    )(info, q_r, do_r, k_str, v_str, kv_win)


def halo_pairs(i, back):
    pairs = []
    for g in range(15):
        for c in range(2):
            src, dst = g * 8 + 6 + c, (g + 1) * 8 + 2 * i + c
            pairs.append((dst, src) if back else (src, dst))
    return pairs


def solution(mesh):
    spec = P('dp', 'cp', None, None)

    def layer(q_rope, k_rope, values, d_out):
        me = lax.axis_index('cp')
        core, x, y, z = me % 2, (me // 2) % NX, (me // 8) % 4, me // 32
        half = jnp.where(z >= 2, 1, 0)
        zp = jnp.where(z >= 2, 3 - z, z)
        g_kv = x // 2
        a2a = functools.partial(lax.all_to_all, axis_name='cp', split_axis=0, concat_axis=0, tiled=True)

        def pack(a):
            a = a[0].reshape(2, HALF, NX, TRIPLE, 128)
            return a.transpose(0, 2, 3, 1, 4).reshape(8, TRIPLE, HALF, 128)

        kv = jnp.stack([k_rope[0], values[0]])
        kv = kv.transpose(2, 0, 1, 3)

        blocks = kv.reshape(2, 2, STRIDE, BLOCK, 128)
        sent = jnp.stack([jnp.stack([blocks[t // 2, :, residue(TRIPLE * t + u)] for u in range(TRIPLE)]) for t in range(NX)])
        mine = a2a(sent, axis_index_groups=GROUP_X)
        gathered = []
        for u in range(TRIPLE):
            gathered.append(lax.all_gather(mine[:, u].transpose(1, 0, 2, 3), 'cp', axis=1, axis_index_groups=GROUP_ZYC))

        q_r = a2a(pack(q_rope), axis_index_groups=GROUP_Q)
        do_r = a2a(pack(d_out), axis_index_groups=GROUP_Q)

        piece = jnp.zeros((2, 2, 128, 128), BF16)
        for i in range(NX):
            piece = piece + lax.ppermute(kv[:, :, i * 128:(i + 1) * 128], 'cp', halo_pairs(i, False))
        ext = jnp.concatenate([kv, piece], axis=2)
        keep = lax.dynamic_index_in_dim(ext, g_kv, axis=0, keepdims=False)
        got = lax.ppermute(lax.dynamic_index_in_dim(ext, 1 - g_kv, axis=0, keepdims=False), 'cp', [(d, d ^ 4) for d in range(128)])
        two = jnp.stack([jnp.where(g_kv == 0, keep, got), jnp.where(g_kv == 0, got, keep)])
        allw = lax.all_gather(two, 'cp', axis=0, axis_index_groups=GROUP_WG)
        sel = allw.reshape(2, 2, 2, 2, 2, 640, 128)
        body = sel[:, :, :, :, :, :RUN].transpose(0, 4, 3, 1, 2, 5, 6).reshape(2, 2, 4096, 128)
        head_part = sel[:, :, :, :, :, RUN:].transpose(0, 4, 2, 3, 1, 5, 6).reshape(2, 2, HALO, 128)
        kv_win = jnp.concatenate([head_part, body], axis=2)

        member = half * NX + x

        def swap(parts):
            got = []
            for k in range(8):
                part = lax.dynamic_index_in_dim(parts, member ^ k, axis=0, keepdims=False)
                if k:
                    part = lax.ppermute(part, 'cp', [(g[m], g[m ^ k]) for g in GROUP_Q for m in range(8)])
                got.append(part)
            return got

        outs = []
        str_sum = []
        win_sum = None
        for u in range(TRIPLE):
            res = (-1 - (TRIPLE * x + u)) % STRIDE
            info = jnp.stack([4 * zp + y, 4 * (3 - zp) + y, core, half, res, 0, 0, 0]).astype(jnp.int32)
            o, dq, dkv, dkw = head_attention(info, q_r, do_r, gathered[u][0], gathered[u][1], kv_win, u)
            outs.append(swap(jnp.stack([o, dq], axis=1)))
            back = a2a(dkv, axis_index_groups=GROUP_ZYC)
            str_sum.append(jnp.sum(back, axis=0, dtype=F32))
            win_sum = dkw if win_sum is None else win_sum + dkw

        both = jnp.stack([jnp.stack(o) for o in outs], axis=1)
        both = jnp.stack([lax.dynamic_index_in_dim(both, member ^ j, axis=0, keepdims=False) for j in range(8)])
        both = both.reshape(2, NX, TRIPLE, 2, HALF, 128).transpose(3, 0, 4, 1, 2, 5).reshape(2, RUN, 12, 128)

        body = win_sum[:, :, HALO:].reshape(2, 2, NX, 2, RUN, 128).transpose(0, 2, 3, 1, 4, 5)
        head_part = win_sum[:, :, :HALO].reshape(2, 2, 2, NX, 128, 128).transpose(0, 3, 2, 1, 4, 5)
        wsend = jnp.concatenate([body, head_part], axis=4).reshape(16, 2, 640, 128).astype(BF16)
        wgot = a2a(wsend, axis_index_groups=GROUP_W).reshape(2, 2, 2, 2, 2, 640, 128)
        wtot = jnp.sum(wgot, axis=(0, 2, 3), dtype=F32)
        grads = wtot[:, :, :RUN]
        pieces = [lax.ppermute(wtot[:, :, RUN:], 'cp', halo_pairs(i, True)) for i in range(NX)]
        grads = grads + jnp.concatenate(pieces, axis=2)

        home = a2a(jnp.stack(str_sum).transpose(2, 0, 1, 3, 4), axis_index_groups=GROUP_X)
        by_kv = []
        for g in range(2):
            slots = [jnp.zeros((2, BLOCK, 128), F32)] * STRIDE
            for h in range(6 * g, 6 * g + 6):
                slots[residue(h)] = home[h // TRIPLE, h % TRIPLE]
            by_kv.append(jnp.concatenate(slots, axis=1))
        grads = (grads + jnp.stack(by_kv)).astype(BF16)
        grads = grads.transpose(1, 2, 0, 3)
        return both[0][None], both[1][None], grads[0][None], grads[1][None]

    return jax.shard_map(layer, mesh=mesh, in_specs=(spec, spec, spec, spec), out_specs=(spec, spec, spec, spec), check_vma=False)
```

```python
import functools
import math

import jax
import jax.numpy as jnp
from jax import lax
from jax.experimental import pallas as pl
from jax.experimental.pallas import tpu as pltpu
from jax.sharding import PartitionSpec as P


BLOCK = 64
LOCAL = 16
STRIDE = 8
NX = 4
TRIPLE = 3
HALF = 256
RUN = 512
HALO = 1024
PER = 4
CHUNK = 512 * PER
SUBG = 1
SUB = 512 * SUBG
WIN = (LOCAL - 1) * BLOCK + HALF
WSUB = ((0, 7), (7, 13), (13, 19))
F32 = jnp.float32
BF16 = jnp.bfloat16


def dev(z, y, x, c):
    return ((z * 4 + y) * NX + x) * 2 + c


def zof(zp, zm):
    return zp if zm == 0 else 3 - zp


GROUP_Q = [[dev(zof(zp, zm), y, x, c) for zm in range(2) for x in range(NX)] for zp in range(2) for y in range(4) for c in range(2)]
GROUP_X = [[dev(z, y, x, c) for x in range(NX)] for z in range(4) for y in range(4) for c in range(2)]
GROUP_ZYC = [[dev(z, y, x, c) for z in range(4) for y in range(4) for c in range(2)] for x in range(NX)]
GROUP_WG = [[dev(zof(zp, zm), y, 2 * xh + xl, c) for zm in range(2) for xl in range(2)] for zp in range(2) for y in range(4) for xh in range(2) for c in range(2)]


def residue(head):
    return (-1 - head) % STRIDE


def nt(a, b):
    return lax.dot_general(a, b, (((1,), (1,)), ((), ())), preferred_element_type=F32)


def tn(a, b):
    return lax.dot_general(a, b, (((0,), (0,)), ((), ())), preferred_element_type=F32)


def nn(a, b):
    return lax.dot_general(a, b, (((1,), (0,)), ((), ())), preferred_element_type=F32)


def attn_kernel(chained, info, q_ref, do_ref, ks_ref, vs_ref, kw_ref, *refs):
    prev_ref = refs[0] if chained else None
    oq_ref, dkv_ref, dkw_ref, e_s, dp_s, m_s, e_l, dp_l, dk_s, dv_s = refs[chained:]
    tile = pl.program_id(0)
    member = tile // NX
    xsrc = tile % NX
    scale = 1.0 / 128
    cexp = scale * math.log2(math.e)
    group = info[member]
    core = info[2]
    half = info[3]
    res = info[4]
    t0 = RUN * (2 * xsrc + core) + HALF * half
    blk0 = group * 64 + t0 // BLOCK
    q = q_ref[0, 0]
    do = do_ref[0, 0]

    @pl.when(tile == 0)
    def _():
        dk_s[...] = jnp.zeros_like(dk_s)
        dv_s[...] = jnp.zeros_like(dv_s)

    @pl.when(xsrc == 0)
    def _():
        if chained:
            pltpu.sync_copy(prev_ref.at[member], dkw_ref.at[0])
        else:
            dkw_ref[...] = jnp.zeros_like(dkw_ref)

    qblk = lax.broadcasted_iota(jnp.int32, (1, HALF), 1) // BLOCK

    def mask_slots(s, masks):
        return jnp.concatenate([jnp.where(mk, s[BLOCK * i:BLOCK * (i + 1)], -jnp.inf) for i, mk in enumerate(masks)], axis=0)

    def stats(s, dp, m, l, d):
        m_new = jnp.maximum(m, jnp.max(s, axis=0, keepdims=True))
        e = jnp.exp2((s - m_new) * cexp)
        a = jnp.exp2((m - m_new) * cexp)
        l = l * a + jnp.sum(e, axis=0, keepdims=True)
        d = d * a + jnp.sum(e * dp, axis=0, keepdims=True)
        return e, m_new, l, d

    nb = WIN // BLOCK
    masks = [(qblk <= min(i, 4)) & (blk0 - (LOCAL - 1) + i >= 0) for i in range(nb)]
    kr = lax.broadcasted_iota(jnp.int32, (HALF, HALF), 0)
    qc = lax.broadcasted_iota(jnp.int32, (HALF, HALF), 1)
    m, l, d = jnp.full((1, HALF), -jnp.inf, F32), jnp.zeros((1, HALF), F32), jnp.zeros((1, HALF), F32)
    m_l = []
    for lo, hi in reversed(WSUB):
        rows = pl.ds(pl.multiple_of(t0 + BLOCK * (lo + 1), BLOCK), BLOCK * (hi - lo))
        s = nt(kw_ref[0, 0, rows], q)
        dp = nt(kw_ref[0, 1, rows], do)
        if hi == nb:
            cut = BLOCK * (hi - lo) - HALF
            s = jnp.concatenate([mask_slots(s[:cut], masks[lo:hi - 4]), jnp.where(kr <= qc, s[cut:], -jnp.inf)], axis=0)
        else:
            s = mask_slots(s, masks[lo:hi])
        e, m, l, d = stats(s, dp, m, l, d)
        e_l[BLOCK * lo:BLOCK * hi] = e
        dp_l[BLOCK * lo:BLOCK * hi] = dp
        m_l.append(m)
    m_l.reverse()

    limit = blk0 - LOCAL - res

    def keys(ref, i):
        return ref[pl.ds(2 * PER * i, 2 * PER), 0].reshape(CHUNK, 128)

    def part(ref, i, n):
        return ref[pl.ds(2 * PER * i + 2 * SUBG * n, 2 * SUBG), 0].reshape(SUB, 128)

    def score(i, carry, masked):
        m, l, d = carry
        for n in range(PER // SUBG):
            s = nt(part(ks_ref, i, n), q)
            dp = nt(part(vs_ref, i, n), do)
            if masked:
                first = [64 * (PER * i + SUBG * n + b // 8) + 8 * (2 * (b % NX) + b % 8 // NX) for b in range(SUB // BLOCK)]
                s = mask_slots(s, [qblk >= f - limit for f in first])
            e, m, l, d = stats(s, dp, m, l, d)
            e_s[i, n] = e
            dp_s[i, n] = dp
            m_s[i, n] = jnp.broadcast_to(m, (8, HALF))
        return m, l, d

    n_open = jnp.maximum(group - 1, 0) // PER
    n_all = (group + PER) // PER
    carry = lax.fori_loop(0, n_open, functools.partial(score, masked=False), (m, l, d))
    m, l, d = lax.fori_loop(n_open, n_all, functools.partial(score, masked=True), carry)
    inv = 1.0 / l
    delta = d * inv

    def weights(e, dp, m_old):
        p = e * (jnp.exp2((m_old - m) * cexp) * inv)
        return p.astype(BF16), (p * (dp - delta)).astype(BF16)

    win = pl.ds(pl.multiple_of(t0 + BLOCK, BLOCK), WIN)
    pairs = [weights(e_l[BLOCK * lo:BLOCK * hi], dp_l[BLOCK * lo:BLOCK * hi], m_l[n]) for n, (lo, hi) in enumerate(WSUB)]
    pb = jnp.concatenate([p for p, _ in pairs], axis=0)
    ds = jnp.concatenate([g for _, g in pairs], axis=0)
    ot = tn(kw_ref[0, 1, win], pb)
    dqt = tn(kw_ref[0, 0, win], ds)
    dkw_ref[0, 1, win] += nn(pb, do)
    dkw_ref[0, 0, win] += nn(ds, q) * scale

    def grad(i, carry):
        ot, dqt = carry
        pairs = [weights(e_s[i, n], dp_s[i, n], m_s[i, n][0:1]) for n in range(PER // SUBG)]
        pb = jnp.concatenate([p for p, _ in pairs], axis=0)
        ds = jnp.concatenate([g for _, g in pairs], axis=0)
        rows = pl.ds(pl.multiple_of(i * CHUNK, CHUNK), CHUNK)
        dv_s[rows] += nn(pb, do)
        dk_s[rows] += nn(ds, q)
        return ot + tn(keys(vs_ref, i), pb), dqt + tn(keys(ks_ref, i), ds)

    ot, dqt = lax.fori_loop(0, n_all, grad, (ot, dqt))
    oq_ref[0, 0] = ot.T.astype(BF16)
    oq_ref[0, 1] = (dqt * scale).T.astype(BF16)

    @pl.when(tile == pl.num_programs(0) - 1)
    def _():
        dkv_ref[:, 0] = (dk_s[...] * scale).astype(BF16).reshape(32, NX, BLOCK, 128)
        dkv_ref[:, 1] = dv_s[...].astype(BF16).reshape(32, NX, BLOCK, 128)


def head_attention(info, qd_r, kv_str, kv_win, prev, u):
    def whole(n):
        return pl.BlockSpec((32, 1, NX, BLOCK, 128), lambda t, s: (0, n, 0, 0, 0), pipeline_mode=pl.Buffered(1))

    def qspec(n):
        return pl.BlockSpec((1, 1, HALF, 128), lambda t, s: (t, n, 0, 0))

    wspec = pl.BlockSpec((1, 2, HALO + 4096, 128), lambda t, s: (t // NX, 0, 0, 0))
    pairs = 2048 * 5400
    chained = prev is not None
    return pl.pallas_call(
        functools.partial(attn_kernel, chained),
        grid_spec=pltpu.PrefetchScalarGridSpec(
            num_scalar_prefetch=1,
            grid=(8,),
            in_specs=[qspec(u), qspec(TRIPLE + u), whole(0), whole(1), wspec] + [pl.BlockSpec(memory_space=pl.ANY)] * chained,
            out_specs=[pl.BlockSpec((1, 2, HALF, 128), lambda t, s: (t ^ s[5], 0, 0, 0)),
                       pl.BlockSpec((32, 2, NX, BLOCK, 128), lambda t, s: (0, 0, 0, 0, 0)),
                       wspec],
            scratch_shapes=[
                pltpu.VMEM((16 // PER, PER // SUBG, SUB, HALF), F32),
                pltpu.VMEM((16 // PER, PER // SUBG, SUB, HALF), F32),
                pltpu.VMEM((16 // PER, PER // SUBG, 8, HALF), F32),
                pltpu.VMEM((WIN, HALF), F32),
                pltpu.VMEM((WIN, HALF), F32),
                pltpu.VMEM((8192, 128), F32),
                pltpu.VMEM((8192, 128), F32),
            ],
        ),
        out_shape=[jax.ShapeDtypeStruct((8, 2, HALF, 128), BF16),
                   jax.ShapeDtypeStruct((32, 2, NX, BLOCK, 128), BF16),
                   jax.ShapeDtypeStruct(kv_win.shape, F32)],
        compiler_params=pltpu.CompilerParams(vmem_limit_bytes=62 * 1024 * 1024),
        cost_estimate=pl.CostEstimate(flops=pairs * 6 * 256, bytes_accessed=40 * 1024 * 1024, transcendentals=pairs),
        name='head_attention',
    )(info, qd_r, qd_r, kv_str, kv_str, kv_win, *([prev] if chained else []))


def halo_pairs(i, back):
    pairs = []
    for g in range(15):
        for c in range(2):
            src, dst = g * 8 + 6 + c, (g + 1) * 8 + 2 * i + c
            pairs.append((dst, src) if back else (src, dst))
    return pairs


def solution(mesh):
    spec = P('dp', 'cp', None, None)

    def layer(q_rope, k_rope, values, d_out):
        me = lax.axis_index('cp')
        core, x, y, z = me % 2, (me // 2) % NX, (me // 8) % 4, me // 32
        half = jnp.where(z >= 2, 1, 0)
        zp = jnp.where(z >= 2, 3 - z, z)
        g_kv = x // 2
        a2a = functools.partial(lax.all_to_all, axis_name='cp', split_axis=0, concat_axis=0, tiled=True)

        mate = [(d, d ^ 1) for d in range(128)]

        def pack(a):
            a = a[0].reshape(2, HALF, NX, TRIPLE, 128)
            return a.transpose(0, 2, 3, 1, 4).reshape(8, TRIPLE, HALF, 128)

        kv = jnp.stack([k_rope[0], values[0]])
        kv = kv.transpose(2, 0, 1, 3)

        blocks = kv.reshape(2, 2, STRIDE, BLOCK, 128)
        sent = jnp.stack([jnp.stack([blocks[t // 2, :, residue(TRIPLE * t + u)] for u in range(TRIPLE)]) for t in range(NX)])
        mine = a2a(sent, axis_index_groups=GROUP_X)
        mate = [(dev_id, dev_id ^ 1) for dev_id in range(128)]

        gathered = []
        for u in range(TRIPLE):
            gathered.append(lax.all_gather(mine[:, u].transpose(1, 0, 2, 3), 'cp', axis=0, axis_index_groups=GROUP_ZYC))

        qd_r = a2a(jnp.concatenate([pack(q_rope), pack(d_out)], axis=1), axis_index_groups=GROUP_Q)

        piece = jnp.zeros((2, 2, 128, 128), BF16)
        for i in range(NX):
            piece = piece + lax.ppermute(kv[:, :, i * 128:(i + 1) * 128], 'cp', halo_pairs(i, False))
        ext = jnp.concatenate([kv, piece], axis=2)
        keep = lax.dynamic_index_in_dim(ext, g_kv, axis=0, keepdims=False)
        got = lax.ppermute(lax.dynamic_index_in_dim(ext, 1 - g_kv, axis=0, keepdims=False), 'cp', [(d, d ^ 4) for d in range(128)])
        two = jnp.stack([jnp.where(g_kv == 0, keep, got), jnp.where(g_kv == 0, got, keep)])
        spot = half * 2 + x % 2
        allw = jnp.stack([two] + [lax.ppermute(two, 'cp', [(g[m], g[m ^ k]) for g in GROUP_WG for m in range(4)]) for k in range(1, 4)])
        allw = jnp.stack([lax.dynamic_index_in_dim(allw, spot ^ j, axis=0, keepdims=False) for j in range(4)])
        mate_w = lax.ppermute(allw, 'cp', mate)
        sel = jnp.stack([jnp.where(core == 0, allw, mate_w), jnp.where(core == 0, mate_w, allw)], axis=1)
        sel = sel.reshape(2, 2, 2, 2, 2, 640, 128)
        body = sel[:, :, :, :, :, :RUN].transpose(0, 4, 3, 1, 2, 5, 6).reshape(2, 2, 4096, 128)
        head_part = sel[:, :, :, :, :, RUN:].transpose(0, 4, 2, 3, 1, 5, 6).reshape(2, 2, HALO, 128)
        kv_win = jnp.concatenate([head_part, body], axis=2)

        member = half * NX + x

        def swap(parts):
            return [parts[0]] + [lax.ppermute(parts[k], 'cp', [(g[m], g[m ^ k]) for g in GROUP_Q for m in range(8)]) for k in range(1, 8)]

        outs = []
        str_sum = []
        dkw = None
        for u in range(TRIPLE):
            res = (-1 - (TRIPLE * x + u)) % STRIDE
            info = jnp.stack([4 * zp + y, 4 * (3 - zp) + y, core, half, res, member, 0, 0]).astype(jnp.int32)
            oq, dkv, dkw = head_attention(info, qd_r, gathered[u], kv_win, dkw, u)
            back = a2a(dkv, axis_index_groups=GROUP_ZYC)
            str_sum.append(jnp.sum(back, axis=0, dtype=F32))
            outs.append(oq)

        first = swap([jnp.stack([outs[0][k], outs[1][k]]) for k in range(8)])
        last = swap([outs[2][k] for k in range(8)])
        both = jnp.stack([jnp.concatenate([f, t[None]]) for f, t in zip(first, last)])
        both = jnp.stack([lax.dynamic_index_in_dim(both, member ^ j, axis=0, keepdims=False) for j in range(8)])
        both = both.reshape(2, NX, TRIPLE, 2, HALF, 128).transpose(3, 0, 4, 1, 2, 5).reshape(2, RUN, 12, 128)

        def core_body(c):
            return lax.dynamic_index_in_dim(dkw[:, :, HALO:].reshape(2, 2, NX, 2, RUN, 128), c, axis=3, keepdims=False).transpose(0, 2, 1, 3, 4)

        def core_head(c):
            return lax.dynamic_index_in_dim(dkw[:, :, :HALO].reshape(2, 2, 2, NX, 128, 128), c, axis=2, keepdims=False).transpose(0, 2, 1, 3, 4)

        def owners(part, rows):
            other = lax.ppermute(part(1 - core).reshape(8, 2, rows, 128), 'cp', mate)
            total = (part(core).reshape(8, 2, rows, 128) + other).astype(BF16)
            got = swap([lax.dynamic_index_in_dim(total, member ^ k, axis=0, keepdims=False) for k in range(8)])
            same, cross = [sum(got[k].astype(F32) for k in range(8) if k // 2 % 2 == n) for n in range(2)]
            return jnp.stack([jnp.where(g_kv == 0, same, cross), jnp.where(g_kv == 0, cross, same)])

        head_sum = owners(core_head, 128)
        grads = owners(core_body, RUN)
        pieces = [lax.ppermute(head_sum, 'cp', halo_pairs(i, True)) for i in range(NX)]
        grads = grads + jnp.concatenate(pieces, axis=2)

        owned = jnp.stack(str_sum).transpose(2, 0, 1, 3, 4)
        owned = [lax.dynamic_index_in_dim(owned, x ^ k, axis=0, keepdims=False) for k in range(NX)]
        owned = jnp.stack([owned[0]] + [lax.ppermute(owned[k], 'cp', [(g[m], g[m ^ k]) for g in GROUP_X for m in range(NX)]) for k in range(1, NX)])
        home = [lax.dynamic_index_in_dim(owned, x ^ t, axis=0, keepdims=False) for t in range(NX)]
        by_kv = []
        for g in range(2):
            slots = [jnp.zeros((2, BLOCK, 128), F32)] * STRIDE
            for h in range(6 * g, 6 * g + 6):
                slots[residue(h)] = home[h // TRIPLE][h % TRIPLE]
            by_kv.append(jnp.concatenate(slots, axis=1))
        grads = (grads + jnp.stack(by_kv)).astype(BF16)
        grads = grads.transpose(1, 2, 0, 3)
        return both[0][None], both[1][None], grads[0][None], grads[1][None]

    return jax.shard_map(layer, mesh=mesh, in_specs=(spec, spec, spec, spec), out_specs=(spec, spec, spec, spec), check_vma=False)
```

```python
import functools
import math

import jax
import jax.numpy as jnp
from jax import lax
from jax.experimental import pallas as pl
from jax.experimental.pallas import tpu as pltpu
from jax.sharding import PartitionSpec as P


BLOCK = 64
LOCAL = 16
STRIDE = 8
NX = 4
TRIPLE = 3
HALF = 256
RUN = 512
HALO = 1024
PER = 4
CHUNK = 512 * PER
SUBG = 1
SUB = 512 * SUBG
WIN = (LOCAL - 1) * BLOCK + HALF
WSUB = ((0, 7), (7, 13), (13, 19))
F32 = jnp.float32
BF16 = jnp.bfloat16


def dev(z, y, x, c):
    return ((z * 4 + y) * NX + x) * 2 + c


def zof(zp, zm):
    return zp if zm == 0 else 3 - zp


GROUP_Q = [[dev(zof(zp, zm), y, x, c) for zm in range(2) for x in range(NX)] for zp in range(2) for y in range(4) for c in range(2)]
GROUP_X = [[dev(z, y, x, c) for x in range(NX)] for z in range(4) for y in range(4) for c in range(2)]
GROUP_ZYC = [[dev(z, y, x, c) for z in range(4) for y in range(4) for c in range(2)] for x in range(NX)]
GROUP_WG = [[dev(zof(zp, zm), y, 2 * xh + xl, c) for zm in range(2) for xl in range(2)] for zp in range(2) for y in range(4) for xh in range(2) for c in range(2)]


def residue(head):
    return (-1 - head) % STRIDE


def nt(a, b):
    return lax.dot_general(a, b, (((1,), (1,)), ((), ())), preferred_element_type=F32)


def tn(a, b):
    return lax.dot_general(a, b, (((0,), (0,)), ((), ())), preferred_element_type=F32)


def nn(a, b):
    return lax.dot_general(a, b, (((1,), (0,)), ((), ())), preferred_element_type=F32)


def attn_kernel(chained, info, q_ref, do_ref, ks_ref, vs_ref, kw_ref, *refs):
    prev_ref = refs[0] if chained else None
    oq_ref, dkv_ref, dkw_ref, e_s, dp_s, m_s, e_l, dp_l, dk_s, dv_s, prev_sem = refs[chained:]
    tile = pl.program_id(0)
    member = tile // NX
    xsrc = tile % NX
    scale = 1.0 / 128
    cexp = scale * math.log2(math.e)
    group = info[member]
    core = info[2]
    half = info[3]
    res = info[4]
    t0 = RUN * (2 * xsrc + core) + HALF * half
    blk0 = group * 64 + t0 // BLOCK
    q = q_ref[0, 0]
    do = do_ref[0, 0]

    @pl.when(tile == 0)
    def _():
        dk_s[...] = jnp.zeros_like(dk_s)
        dv_s[...] = jnp.zeros_like(dv_s)

    @pl.when(xsrc == 0)
    def _():
        if chained:
            pltpu.make_async_copy(prev_ref.at[member], dkw_ref.at[0], prev_sem).start()
        else:
            dkw_ref[...] = jnp.zeros_like(dkw_ref)

    qblk = lax.broadcasted_iota(jnp.int32, (1, HALF), 1) // BLOCK

    def mask_slots(s, masks):
        return jnp.concatenate([jnp.where(mk, s[BLOCK * i:BLOCK * (i + 1)], -jnp.inf) for i, mk in enumerate(masks)], axis=0)

    def stats(s, dp, m, l, d):
        m_new = jnp.maximum(m, jnp.max(s, axis=0, keepdims=True))
        e = jnp.exp2((s - m_new) * cexp)
        a = jnp.exp2((m - m_new) * cexp)
        l = l * a + jnp.sum(e, axis=0, keepdims=True)
        d = d * a + jnp.sum(e * dp, axis=0, keepdims=True)
        return e, m_new, l, d

    nb = WIN // BLOCK
    masks = [(qblk <= min(i, 4)) & (blk0 - (LOCAL - 1) + i >= 0) for i in range(nb)]
    kr = lax.broadcasted_iota(jnp.int32, (HALF, HALF), 0)
    qc = lax.broadcasted_iota(jnp.int32, (HALF, HALF), 1)
    m, l, d = jnp.full((1, HALF), -jnp.inf, F32), jnp.zeros((1, HALF), F32), jnp.zeros((1, HALF), F32)
    m_l = []
    for lo, hi in reversed(WSUB):
        rows = pl.ds(pl.multiple_of(t0 + BLOCK * (lo + 1), BLOCK), BLOCK * (hi - lo))
        s = nt(kw_ref[0, 0, rows], q)
        dp = nt(kw_ref[0, 1, rows], do)
        if hi == nb:
            cut = BLOCK * (hi - lo) - HALF
            s = jnp.concatenate([mask_slots(s[:cut], masks[lo:hi - 4]), jnp.where(kr <= qc, s[cut:], -jnp.inf)], axis=0)
        else:
            s = mask_slots(s, masks[lo:hi])
        e, m, l, d = stats(s, dp, m, l, d)
        e_l[BLOCK * lo:BLOCK * hi] = e
        dp_l[BLOCK * lo:BLOCK * hi] = dp
        m_l.append(m)
    m_l.reverse()

    limit = blk0 - LOCAL - res

    def keys(ref, i):
        return ref[pl.ds(2 * PER * i, 2 * PER), 0].reshape(CHUNK, 128)

    def part(ref, i, n):
        return ref[pl.ds(2 * PER * i + 2 * SUBG * n, 2 * SUBG), 0].reshape(SUB, 128)

    def score(i, carry, masked):
        m, l, d = carry
        for n in range(PER // SUBG):
            s = nt(part(ks_ref, i, n), q)
            dp = nt(part(vs_ref, i, n), do)
            if masked:
                first = [64 * (PER * i + SUBG * n + b // 8) + 8 * (2 * (b % NX) + b % 8 // NX) for b in range(SUB // BLOCK)]
                s = mask_slots(s, [qblk >= f - limit for f in first])
            e, m, l, d = stats(s, dp, m, l, d)
            e_s[i, n] = e
            dp_s[i, n] = dp
            m_s[i, n] = jnp.broadcast_to(m, (8, HALF))
        return m, l, d

    n_open = jnp.maximum(group - 1, 0) // PER
    n_all = (group + PER) // PER
    carry = lax.fori_loop(0, n_open, functools.partial(score, masked=False), (m, l, d))
    m, l, d = lax.fori_loop(n_open, n_all, functools.partial(score, masked=True), carry)
    inv = 1.0 / l
    delta = d * inv

    def weights(e, dp, m_old):
        p = e * (jnp.exp2((m_old - m) * cexp) * inv)
        return p.astype(BF16), (p * (dp - delta)).astype(BF16)

    win = pl.ds(pl.multiple_of(t0 + BLOCK, BLOCK), WIN)
    pairs = [weights(e_l[BLOCK * lo:BLOCK * hi], dp_l[BLOCK * lo:BLOCK * hi], m_l[n]) for n, (lo, hi) in enumerate(WSUB)]
    pb = jnp.concatenate([p for p, _ in pairs], axis=0)
    ds = jnp.concatenate([g for _, g in pairs], axis=0)
    if chained:
        @pl.when(xsrc == 0)
        def _():
            pltpu.make_async_copy(prev_ref.at[member], dkw_ref.at[0], prev_sem).wait()

    ot = tn(kw_ref[0, 1, win], pb)
    dqt = tn(kw_ref[0, 0, win], ds)
    dkw_ref[0, 1, win] += nn(pb, do)
    dkw_ref[0, 0, win] += nn(ds, q) * scale

    def grad(i, carry):
        ot, dqt = carry
        pairs = [weights(e_s[i, n], dp_s[i, n], m_s[i, n][0:1]) for n in range(PER // SUBG)]
        pb = jnp.concatenate([p for p, _ in pairs], axis=0)
        ds = jnp.concatenate([g for _, g in pairs], axis=0)
        rows = pl.ds(pl.multiple_of(i * CHUNK, CHUNK), CHUNK)
        dv_s[rows] += nn(pb, do)
        dk_s[rows] += nn(ds, q)
        return ot + tn(keys(vs_ref, i), pb), dqt + tn(keys(ks_ref, i), ds)

    ot, dqt = lax.fori_loop(0, n_all, grad, (ot, dqt))
    oq_ref[0, 0] = ot.T.astype(BF16)
    oq_ref[0, 1] = (dqt * scale).T.astype(BF16)

    @pl.when(tile == pl.num_programs(0) - 1)
    def _():
        dkv_ref[:, 0] = (dk_s[...] * scale).astype(BF16).reshape(32, NX, BLOCK, 128)
        dkv_ref[:, 1] = dv_s[...].astype(BF16).reshape(32, NX, BLOCK, 128)


def head_attention(info, qd_r, kv_str, kv_win, prev, u):
    def whole(n):
        return pl.BlockSpec((32, 1, NX, BLOCK, 128), lambda t, s: (0, n, 0, 0, 0), pipeline_mode=pl.Buffered(1))

    def qspec(n):
        return pl.BlockSpec((1, 1, HALF, 128), lambda t, s: (t, n, 0, 0))

    wspec = pl.BlockSpec((1, 2, HALO + 4096, 128), lambda t, s: (t // NX, 0, 0, 0))
    pairs = 2048 * 5400
    chained = prev is not None
    return pl.pallas_call(
        functools.partial(attn_kernel, chained),
        grid_spec=pltpu.PrefetchScalarGridSpec(
            num_scalar_prefetch=1,
            grid=(8,),
            in_specs=[qspec(u), qspec(TRIPLE + u), whole(0), whole(1), wspec] + [pl.BlockSpec(memory_space=pl.ANY)] * chained,
            out_specs=[pl.BlockSpec((1, 2, HALF, 128), lambda t, s: (t ^ s[5], 0, 0, 0)),
                       pl.BlockSpec((32, 2, NX, BLOCK, 128), lambda t, s: (0, 0, 0, 0, 0)),
                       wspec],
            scratch_shapes=[
                pltpu.VMEM((16 // PER, PER // SUBG, SUB, HALF), F32),
                pltpu.VMEM((16 // PER, PER // SUBG, SUB, HALF), F32),
                pltpu.VMEM((16 // PER, PER // SUBG, 8, HALF), F32),
                pltpu.VMEM((WIN, HALF), F32),
                pltpu.VMEM((WIN, HALF), F32),
                pltpu.VMEM((8192, 128), F32),
                pltpu.VMEM((8192, 128), F32),
                pltpu.SemaphoreType.DMA,
            ],
        ),
        out_shape=[jax.ShapeDtypeStruct((8, 2, HALF, 128), BF16),
                   jax.ShapeDtypeStruct((32, 2, NX, BLOCK, 128), BF16),
                   jax.ShapeDtypeStruct(kv_win.shape, F32)],
        compiler_params=pltpu.CompilerParams(vmem_limit_bytes=62 * 1024 * 1024),
        cost_estimate=pl.CostEstimate(flops=pairs * 6 * 256, bytes_accessed=40 * 1024 * 1024, transcendentals=pairs),
        name='head_attention',
    )(info, qd_r, qd_r, kv_str, kv_str, kv_win, *([prev] if chained else []))


def halo_pairs(i, back):
    pairs = []
    for g in range(15):
        for c in range(2):
            src, dst = g * 8 + 6 + c, (g + 1) * 8 + 2 * i + c
            pairs.append((dst, src) if back else (src, dst))
    return pairs


def solution(mesh):
    spec = P('dp', 'cp', None, None)

    def layer(q_rope, k_rope, values, d_out):
        me = lax.axis_index('cp')
        core, x, y, z = me % 2, (me // 2) % NX, (me // 8) % 4, me // 32
        half = jnp.where(z >= 2, 1, 0)
        zp = jnp.where(z >= 2, 3 - z, z)
        g_kv = x // 2
        a2a = functools.partial(lax.all_to_all, axis_name='cp', split_axis=0, concat_axis=0, tiled=True)

        mate = [(d, d ^ 1) for d in range(128)]

        def pack(a):
            a = a[0].reshape(2, HALF, NX, TRIPLE, 128)
            return a.transpose(0, 2, 3, 1, 4).reshape(8, TRIPLE, HALF, 128)

        kv = jnp.stack([k_rope[0], values[0]])
        kv = kv.transpose(2, 0, 1, 3)

        blocks = kv.reshape(2, 2, STRIDE, BLOCK, 128)
        sent = jnp.stack([jnp.stack([blocks[t // 2, :, residue(TRIPLE * t + u)] for u in range(TRIPLE)]) for t in range(NX)])
        mine = a2a(sent, axis_index_groups=GROUP_X)
        mate = [(dev_id, dev_id ^ 1) for dev_id in range(128)]

        gathered = []
        for u in range(TRIPLE):
            gathered.append(lax.all_gather(mine[:, u].transpose(1, 0, 2, 3), 'cp', axis=0, axis_index_groups=GROUP_ZYC))

        qd_r = a2a(jnp.concatenate([pack(q_rope), pack(d_out)], axis=1), axis_index_groups=GROUP_Q)

        piece = jnp.zeros((2, 2, 128, 128), BF16)
        for i in range(NX):
            piece = piece + lax.ppermute(kv[:, :, i * 128:(i + 1) * 128], 'cp', halo_pairs(i, False))
        ext = jnp.concatenate([kv, piece], axis=2)
        keep = lax.dynamic_index_in_dim(ext, g_kv, axis=0, keepdims=False)
        got = lax.ppermute(lax.dynamic_index_in_dim(ext, 1 - g_kv, axis=0, keepdims=False), 'cp', [(d, d ^ 4) for d in range(128)])
        two = jnp.stack([jnp.where(g_kv == 0, keep, got), jnp.where(g_kv == 0, got, keep)])
        spot = half * 2 + x % 2
        allw = jnp.stack([two] + [lax.ppermute(two, 'cp', [(g[m], g[m ^ k]) for g in GROUP_WG for m in range(4)]) for k in range(1, 4)])
        allw = jnp.stack([lax.dynamic_index_in_dim(allw, spot ^ j, axis=0, keepdims=False) for j in range(4)])
        mate_w = lax.ppermute(allw, 'cp', mate)
        sel = jnp.stack([jnp.where(core == 0, allw, mate_w), jnp.where(core == 0, mate_w, allw)], axis=1)
        sel = sel.reshape(2, 2, 2, 2, 2, 640, 128)
        body = sel[:, :, :, :, :, :RUN].transpose(0, 4, 3, 1, 2, 5, 6).reshape(2, 2, 4096, 128)
        head_part = sel[:, :, :, :, :, RUN:].transpose(0, 4, 2, 3, 1, 5, 6).reshape(2, 2, HALO, 128)
        kv_win = jnp.concatenate([head_part, body], axis=2)

        member = half * NX + x

        def swap(parts):
            return [parts[0]] + [lax.ppermute(parts[k], 'cp', [(g[m], g[m ^ k]) for g in GROUP_Q for m in range(8)]) for k in range(1, 8)]

        outs = []
        str_sum = []
        dkw = None
        for u in range(TRIPLE):
            res = (-1 - (TRIPLE * x + u)) % STRIDE
            info = jnp.stack([4 * zp + y, 4 * (3 - zp) + y, core, half, res, member, 0, 0]).astype(jnp.int32)
            oq, dkv, dkw = head_attention(info, qd_r, gathered[u], kv_win, dkw, u)
            back = a2a(dkv, axis_index_groups=GROUP_ZYC)
            str_sum.append(jnp.sum(back, axis=0, dtype=F32))
            outs.append(oq)

        first = swap([jnp.stack([outs[0][k], outs[1][k]]) for k in range(8)])
        last = swap([outs[2][k] for k in range(8)])
        both = jnp.stack([jnp.concatenate([f, t[None]]) for f, t in zip(first, last)])
        both = jnp.stack([lax.dynamic_index_in_dim(both, member ^ j, axis=0, keepdims=False) for j in range(8)])
        both = both.reshape(2, NX, TRIPLE, 2, HALF, 128).transpose(3, 0, 4, 1, 2, 5).reshape(2, RUN, 12, 128)

        def core_body(c):
            return lax.dynamic_index_in_dim(dkw[:, :, HALO:].reshape(2, 2, NX, 2, RUN, 128), c, axis=3, keepdims=False).transpose(0, 2, 1, 3, 4)

        def core_head(c):
            return lax.dynamic_index_in_dim(dkw[:, :, :HALO].reshape(2, 2, 2, NX, 128, 128), c, axis=2, keepdims=False).transpose(0, 2, 1, 3, 4)

        def owners(part, rows):
            other = lax.ppermute(part(1 - core).reshape(8, 2, rows, 128), 'cp', mate)
            total = (part(core).reshape(8, 2, rows, 128) + other).astype(BF16)
            got = swap([lax.dynamic_index_in_dim(total, member ^ k, axis=0, keepdims=False) for k in range(8)])
            same, cross = [sum(got[k].astype(F32) for k in range(8) if k // 2 % 2 == n) for n in range(2)]
            return jnp.stack([jnp.where(g_kv == 0, same, cross), jnp.where(g_kv == 0, cross, same)])

        head_sum = owners(core_head, 128)
        grads = owners(core_body, RUN)
        pieces = [lax.ppermute(head_sum, 'cp', halo_pairs(i, True)) for i in range(NX)]
        grads = grads + jnp.concatenate(pieces, axis=2)

        owned = jnp.stack(str_sum).transpose(2, 0, 1, 3, 4)
        owned = [lax.dynamic_index_in_dim(owned, x ^ k, axis=0, keepdims=False) for k in range(NX)]
        owned = jnp.stack([owned[0]] + [lax.ppermute(owned[k], 'cp', [(g[m], g[m ^ k]) for g in GROUP_X for m in range(NX)]) for k in range(1, NX)])
        home = [lax.dynamic_index_in_dim(owned, x ^ t, axis=0, keepdims=False) for t in range(NX)]
        by_kv = []
        for g in range(2):
            slots = [jnp.zeros((2, BLOCK, 128), F32)] * STRIDE
            for h in range(6 * g, 6 * g + 6):
                slots[residue(h)] = home[h // TRIPLE][h % TRIPLE]
            by_kv.append(jnp.concatenate(slots, axis=1))
        grads = (grads + jnp.stack(by_kv)).astype(BF16)
        grads = grads.transpose(1, 2, 0, 3)
        return both[0][None], both[1][None], grads[0][None], grads[1][None]

    return jax.shard_map(layer, mesh=mesh, in_specs=(spec, spec, spec, spec), out_specs=(spec, spec, spec, spec), check_vma=False)
```

```python
import functools
import math

import jax
import jax.numpy as jnp
from jax import lax
from jax.experimental import pallas as pl
from jax.experimental.pallas import tpu as pltpu
from jax.sharding import PartitionSpec as P


BLOCK = 64
LOCAL = 16
STRIDE = 8
NX = 4
TRIPLE = 3
HALF = 256
RUN = 512
HALO = 1024
PER = 4
CHUNK = 512 * PER
SUBG = 1
SUB = 512 * SUBG
WIN = (LOCAL - 1) * BLOCK + HALF
WSUB = ((0, 7), (7, 13), (13, 19))
F32 = jnp.float32
BF16 = jnp.bfloat16


def dev(z, y, x, c):
    return ((z * 4 + y) * NX + x) * 2 + c


def zof(zp, zm):
    return zp if zm == 0 else 3 - zp


GROUP_Q = [[dev(zof(zp, zm), y, x, c) for zm in range(2) for x in range(NX)] for zp in range(2) for y in range(4) for c in range(2)]
GROUP_X = [[dev(z, y, x, c) for x in range(NX)] for z in range(4) for y in range(4) for c in range(2)]
GROUP_ZYC = [[dev(z, y, x, c) for z in range(4) for y in range(4) for c in range(2)] for x in range(NX)]
GROUP_WG = [[dev(zof(zp, zm), y, 2 * xh + xl, c) for zm in range(2) for xl in range(2)] for zp in range(2) for y in range(4) for xh in range(2) for c in range(2)]


def residue(head):
    return (-1 - head) % STRIDE


def nt(a, b):
    return lax.dot_general(a, b, (((1,), (1,)), ((), ())), preferred_element_type=F32)


def tn(a, b):
    return lax.dot_general(a, b, (((0,), (0,)), ((), ())), preferred_element_type=F32)


def nn(a, b):
    return lax.dot_general(a, b, (((1,), (0,)), ((), ())), preferred_element_type=F32)


def attn_kernel(chained, info, q_ref, do_ref, ks_ref, vs_ref, kw_ref, *refs):
    prev_ref = refs[0] if chained else None
    oq_ref, dkv_ref, dkw_ref, e_s, dp_s, m_s, e_l, dp_l, dk_s, dv_s, prev_sem = refs[chained:]
    tile = pl.program_id(0)
    member = tile // NX
    xsrc = tile % NX
    scale = 1.0 / 128
    cexp = scale * math.log2(math.e)
    group = info[member]
    core = info[2]
    half = info[3]
    res = info[4]
    t0 = RUN * (2 * xsrc + core) + HALF * half
    blk0 = group * 64 + t0 // BLOCK
    q = q_ref[0, 0]
    do = do_ref[0, 0]

    @pl.when(tile == 0)
    def _():
        dk_s[...] = jnp.zeros_like(dk_s)
        dv_s[...] = jnp.zeros_like(dv_s)

    @pl.when(xsrc == 0)
    def _():
        if chained:
            pltpu.make_async_copy(prev_ref.at[member], dkw_ref.at[0], prev_sem).start()
        else:
            dkw_ref[...] = jnp.zeros_like(dkw_ref)

    qblk = lax.broadcasted_iota(jnp.int32, (1, HALF), 1) // BLOCK

    def mask_slots(s, masks):
        return jnp.concatenate([jnp.where(mk, s[BLOCK * i:BLOCK * (i + 1)], -jnp.inf) for i, mk in enumerate(masks)], axis=0)

    def stats(s, dp, m, l, d):
        m_new = jnp.maximum(m, jnp.max(s, axis=0, keepdims=True))
        e = jnp.exp2((s - m_new) * cexp)
        a = jnp.exp2((m - m_new) * cexp)
        l = l * a + jnp.sum(e, axis=0, keepdims=True)
        d = d * a + jnp.sum(e * dp, axis=0, keepdims=True)
        return e, m_new, l, d

    nb = WIN // BLOCK
    masks = [(qblk <= min(i, 4)) & (blk0 - (LOCAL - 1) + i >= 0) for i in range(nb)]
    kr = lax.broadcasted_iota(jnp.int32, (HALF, HALF), 0)
    qc = lax.broadcasted_iota(jnp.int32, (HALF, HALF), 1)
    m, l, d = jnp.full((1, HALF), -jnp.inf, F32), jnp.zeros((1, HALF), F32), jnp.zeros((1, HALF), F32)
    m_l = []
    for lo, hi in reversed(WSUB):
        rows = pl.ds(pl.multiple_of(t0 + BLOCK * (lo + 1), BLOCK), BLOCK * (hi - lo))
        s = nt(kw_ref[0, 0, rows], q)
        dp = nt(kw_ref[0, 1, rows], do)
        if hi == nb:
            cut = BLOCK * (hi - lo) - HALF
            s = jnp.concatenate([mask_slots(s[:cut], masks[lo:hi - 4]), jnp.where(kr <= qc, s[cut:], -jnp.inf)], axis=0)
        else:
            s = mask_slots(s, masks[lo:hi])
        e, m, l, d = stats(s, dp, m, l, d)
        e_l[BLOCK * lo:BLOCK * hi] = e
        dp_l[BLOCK * lo:BLOCK * hi] = dp
        m_l.append(m)
    m_l.reverse()

    limit = blk0 - LOCAL - res

    def keys(ref, i):
        return ref[pl.ds(2 * PER * i, 2 * PER), 0].reshape(CHUNK, 128)

    def part(ref, i, n):
        return ref[pl.ds(2 * PER * i + 2 * SUBG * n, 2 * SUBG), 0].reshape(SUB, 128)

    def score(i, carry, masked):
        m, l, d = carry
        for n in range(PER // SUBG):
            s = nt(part(ks_ref, i, n), q)
            dp = nt(part(vs_ref, i, n), do)
            if masked:
                first = [64 * (PER * i + SUBG * n + b // 8) + 8 * (2 * (b % NX) + b % 8 // NX) for b in range(SUB // BLOCK)]
                s = mask_slots(s, [qblk >= f - limit for f in first])
            e, m, l, d = stats(s, dp, m, l, d)
            e_s[i, n] = e
            dp_s[i, n] = dp
            m_s[i, n] = jnp.broadcast_to(m, (8, HALF))
        return m, l, d

    n_open = jnp.maximum(group - 1, 0) // PER
    n_all = (group + PER) // PER
    carry = lax.fori_loop(0, n_open, functools.partial(score, masked=False), (m, l, d))
    m, l, d = lax.fori_loop(n_open, n_all, functools.partial(score, masked=True), carry)
    inv = 1.0 / l
    delta = d * inv

    def weights(e, dp, m_old):
        p = e * (jnp.exp2((m_old - m) * cexp) * inv)
        return p.astype(BF16), (p * (dp - delta)).astype(BF16)

    win = pl.ds(pl.multiple_of(t0 + BLOCK, BLOCK), WIN)
    pairs = [weights(e_l[BLOCK * lo:BLOCK * hi], dp_l[BLOCK * lo:BLOCK * hi], m_l[n]) for n, (lo, hi) in enumerate(WSUB)]
    pb = jnp.concatenate([p for p, _ in pairs], axis=0)
    ds = jnp.concatenate([g for _, g in pairs], axis=0)
    if chained:
        @pl.when(xsrc == 0)
        def _():
            pltpu.make_async_copy(prev_ref.at[member], dkw_ref.at[0], prev_sem).wait()

    ot = tn(kw_ref[0, 1, win], pb)
    dqt = tn(kw_ref[0, 0, win], ds)
    dkw_ref[0, 1, win] += nn(pb, do)
    dkw_ref[0, 0, win] += nn(ds, q) * scale

    def grad(i, carry):
        ot, dqt = carry
        pairs = [weights(e_s[i, n], dp_s[i, n], m_s[i, n][0:1]) for n in range(PER // SUBG)]
        pb = jnp.concatenate([p for p, _ in pairs], axis=0)
        ds = jnp.concatenate([g for _, g in pairs], axis=0)
        rows = pl.ds(pl.multiple_of(i * CHUNK, CHUNK), CHUNK)
        dv_s[rows] += nn(pb, do)
        dk_s[rows] += nn(ds, q)
        return ot + tn(keys(vs_ref, i), pb), dqt + tn(keys(ks_ref, i), ds)

    ot, dqt = lax.fori_loop(0, n_all, grad, (ot, dqt))
    oq_ref[0, 0] = ot.T.astype(BF16)
    oq_ref[0, 1] = (dqt * scale).T.astype(BF16)

    @pl.when(tile == pl.num_programs(0) - 1)
    def _():
        dkv_ref[:, 0] = (dk_s[...] * scale).astype(BF16).reshape(32, NX, BLOCK, 128)
        dkv_ref[:, 1] = dv_s[...].astype(BF16).reshape(32, NX, BLOCK, 128)


def head_attention(info, qd_r, kv_str, kv_win, prev, u):
    def whole(n):
        return pl.BlockSpec((32, 1, NX, BLOCK, 128), lambda t, s: (0, n, 0, 0, 0), pipeline_mode=pl.Buffered(1))

    def qspec(n):
        return pl.BlockSpec((1, 1, HALF, 128), lambda t, s: (t, n, 0, 0))

    wspec = pl.BlockSpec((1, 2, HALO + 4096, 128), lambda t, s: (t // NX, 0, 0, 0))
    pairs = 2048 * 5400
    chained = prev is not None
    return pl.pallas_call(
        functools.partial(attn_kernel, chained),
        grid_spec=pltpu.PrefetchScalarGridSpec(
            num_scalar_prefetch=1,
            grid=(8,),
            in_specs=[qspec(max(u - 1, 0)), qspec(u + 1), whole(0), whole(1), wspec] + [pl.BlockSpec(memory_space=pl.ANY)] * chained,
            out_specs=[pl.BlockSpec((1, 2, HALF, 128), lambda t, s: (t ^ s[5], 0, 0, 0)),
                       pl.BlockSpec((32, 2, NX, BLOCK, 128), lambda t, s: (0, 0, 0, 0, 0)),
                       wspec],
            scratch_shapes=[
                pltpu.VMEM((16 // PER, PER // SUBG, SUB, HALF), F32),
                pltpu.VMEM((16 // PER, PER // SUBG, SUB, HALF), F32),
                pltpu.VMEM((16 // PER, PER // SUBG, 8, HALF), F32),
                pltpu.VMEM((WIN, HALF), F32),
                pltpu.VMEM((WIN, HALF), F32),
                pltpu.VMEM((8192, 128), F32),
                pltpu.VMEM((8192, 128), F32),
                pltpu.SemaphoreType.DMA,
            ],
        ),
        out_shape=[jax.ShapeDtypeStruct((8, 2, HALF, 128), BF16),
                   jax.ShapeDtypeStruct((32, 2, NX, BLOCK, 128), BF16),
                   jax.ShapeDtypeStruct(kv_win.shape, F32)],
        compiler_params=pltpu.CompilerParams(vmem_limit_bytes=62 * 1024 * 1024),
        cost_estimate=pl.CostEstimate(flops=pairs * 6 * 256, bytes_accessed=40 * 1024 * 1024, transcendentals=pairs),
        name='head_attention',
    )(info, qd_r, qd_r, kv_str, kv_str, kv_win, *([prev] if chained else []))


def halo_pairs(i, back):
    pairs = []
    for g in range(15):
        for c in range(2):
            src, dst = g * 8 + 6 + c, (g + 1) * 8 + 2 * i + c
            pairs.append((dst, src) if back else (src, dst))
    return pairs


def solution(mesh):
    spec = P('dp', 'cp', None, None)

    def layer(q_rope, k_rope, values, d_out):
        me = lax.axis_index('cp')
        core, x, y, z = me % 2, (me // 2) % NX, (me // 8) % 4, me // 32
        half = jnp.where(z >= 2, 1, 0)
        zp = jnp.where(z >= 2, 3 - z, z)
        g_kv = x // 2
        a2a = functools.partial(lax.all_to_all, axis_name='cp', split_axis=0, concat_axis=0, tiled=True)

        mate = [(d, d ^ 1) for d in range(128)]

        def pack(a):
            a = a[0].reshape(2, HALF, NX, TRIPLE, 128)
            return a.transpose(0, 2, 3, 1, 4).reshape(8, TRIPLE, HALF, 128)

        kv = jnp.stack([k_rope[0], values[0]])
        kv = kv.transpose(2, 0, 1, 3)

        blocks = kv.reshape(2, 2, STRIDE, BLOCK, 128)
        sent = jnp.stack([jnp.stack([blocks[t // 2, :, residue(TRIPLE * t + u)] for u in range(TRIPLE)]) for t in range(NX)])
        mine = a2a(sent, axis_index_groups=GROUP_X)
        mate = [(dev_id, dev_id ^ 1) for dev_id in range(128)]

        gathered = []
        for u in range(TRIPLE):
            gathered.append(lax.all_gather(mine[:, u].transpose(1, 0, 2, 3), 'cp', axis=0, axis_index_groups=GROUP_ZYC))

        packed = jnp.stack([pack(q_rope), pack(d_out)], axis=1)
        qd_0 = a2a(packed[:, :, 0], axis_index_groups=GROUP_Q)
        qd_12 = a2a(packed[:, :, 1:].reshape(8, 4, HALF, 128), axis_index_groups=GROUP_Q)

        piece = jnp.zeros((2, 2, 128, 128), BF16)
        for i in range(NX):
            piece = piece + lax.ppermute(kv[:, :, i * 128:(i + 1) * 128], 'cp', halo_pairs(i, False))
        ext = jnp.concatenate([kv, piece], axis=2)
        keep = lax.dynamic_index_in_dim(ext, g_kv, axis=0, keepdims=False)
        got = lax.ppermute(lax.dynamic_index_in_dim(ext, 1 - g_kv, axis=0, keepdims=False), 'cp', [(d, d ^ 4) for d in range(128)])
        two = jnp.stack([jnp.where(g_kv == 0, keep, got), jnp.where(g_kv == 0, got, keep)])
        spot = half * 2 + x % 2
        allw = jnp.stack([two] + [lax.ppermute(two, 'cp', [(g[m], g[m ^ k]) for g in GROUP_WG for m in range(4)]) for k in range(1, 4)])
        allw = jnp.stack([lax.dynamic_index_in_dim(allw, spot ^ j, axis=0, keepdims=False) for j in range(4)])
        mate_w = lax.ppermute(allw, 'cp', mate)
        sel = jnp.stack([jnp.where(core == 0, allw, mate_w), jnp.where(core == 0, mate_w, allw)], axis=1)
        sel = sel.reshape(2, 2, 2, 2, 2, 640, 128)
        body = sel[:, :, :, :, :, :RUN].transpose(0, 4, 3, 1, 2, 5, 6).reshape(2, 2, 4096, 128)
        head_part = sel[:, :, :, :, :, RUN:].transpose(0, 4, 2, 3, 1, 5, 6).reshape(2, 2, HALO, 128)
        kv_win = jnp.concatenate([head_part, body], axis=2)

        member = half * NX + x

        def swap(parts):
            return [parts[0]] + [lax.ppermute(parts[k], 'cp', [(g[m], g[m ^ k]) for g in GROUP_Q for m in range(8)]) for k in range(1, 8)]

        outs = []
        str_sum = []
        dkw = None
        for u in range(TRIPLE):
            res = (-1 - (TRIPLE * x + u)) % STRIDE
            info = jnp.stack([4 * zp + y, 4 * (3 - zp) + y, core, half, res, member, 0, 0]).astype(jnp.int32)
            oq, dkv, dkw = head_attention(info, qd_12 if u else qd_0, gathered[u], kv_win, dkw, u)
            back = a2a(dkv, axis_index_groups=GROUP_ZYC)
            str_sum.append(jnp.sum(back, axis=0, dtype=F32))
            outs.append(oq)

        first = swap([jnp.stack([outs[0][k], outs[1][k]]) for k in range(8)])
        last = swap([outs[2][k] for k in range(8)])
        both = jnp.stack([jnp.concatenate([f, t[None]]) for f, t in zip(first, last)])
        both = jnp.stack([lax.dynamic_index_in_dim(both, member ^ j, axis=0, keepdims=False) for j in range(8)])
        both = both.reshape(2, NX, TRIPLE, 2, HALF, 128).transpose(3, 0, 4, 1, 2, 5).reshape(2, RUN, 12, 128)

        by_pair = dkw.reshape(2, 2, 5, 2, RUN, 128)

        other = lax.ppermute(lax.dynamic_index_in_dim(by_pair, 1 - core, axis=3, keepdims=False), 'cp', mate)
        total = (lax.dynamic_index_in_dim(by_pair, core, axis=3, keepdims=False) + other).astype(BF16)

        def owners(total):
            got = swap([lax.dynamic_index_in_dim(total, member ^ k, axis=0, keepdims=False) for k in range(8)])
            same, cross = [sum(got[k].astype(F32) for k in range(8) if k // 2 % 2 == n) for n in range(2)]
            return jnp.stack([jnp.where(g_kv == 0, same, cross), jnp.where(g_kv == 0, cross, same)])

        head_sum = owners(total[:, :, 0].reshape(2, 2, NX, 128, 128).transpose(0, 2, 1, 3, 4).reshape(8, 2, 128, 128))
        grads = owners(total[:, :, 1:].transpose(0, 2, 1, 3, 4).reshape(8, 2, RUN, 128))
        pieces = [lax.ppermute(head_sum, 'cp', halo_pairs(i, True)) for i in range(NX)]
        grads = grads + jnp.concatenate(pieces, axis=2)

        owned = jnp.stack(str_sum).transpose(2, 0, 1, 3, 4)
        owned = [lax.dynamic_index_in_dim(owned, x ^ k, axis=0, keepdims=False) for k in range(NX)]
        owned = jnp.stack([owned[0]] + [lax.ppermute(owned[k], 'cp', [(g[m], g[m ^ k]) for g in GROUP_X for m in range(NX)]) for k in range(1, NX)])
        home = [lax.dynamic_index_in_dim(owned, x ^ t, axis=0, keepdims=False) for t in range(NX)]
        by_kv = []
        for g in range(2):
            slots = [jnp.zeros((2, BLOCK, 128), F32)] * STRIDE
            for h in range(6 * g, 6 * g + 6):
                slots[residue(h)] = home[h // TRIPLE][h % TRIPLE]
            by_kv.append(jnp.concatenate(slots, axis=1))
        grads = (grads + jnp.stack(by_kv)).astype(BF16)
        grads = grads.transpose(1, 2, 0, 3)
        return both[0][None], both[1][None], grads[0][None], grads[1][None]

    return jax.shard_map(layer, mesh=mesh, in_specs=(spec, spec, spec, spec), out_specs=(spec, spec, spec, spec), check_vma=False)
```
